32 devices in a mesh: row: 4 (over y, core), col: 8 (over z, x).
Axes of the slice: x: 2, y: 2, z: 4, core: 2. Of those that a mesh axis runs over, the one named last changes fastest.
Arguments:
- tokens: bfloat16 [64, 16384], P('row', 'col'), may hold values from -6 to 6
- gate_weight: bfloat16 [16384, 26624], P('col', 'row'), may hold values from -0.046875 to 0.046875
- up_weight: bfloat16 [16384, 26624], P('col', 'row'), may hold values from -0.046875 to 0.046875
Outputs:
- hidden: bfloat16 [64, 26624], P(None, 'row')
The draws below stay inside these ranges and needn't reach their ends.
All inputs are finite; a program needn't handle non-finite values.
Results may differ from the reference program's by a relative error of at most 0.001.
Values may be sent and summed in bfloat16 or wider, within the bound.
A program may use at most 128 MiB of HBM per device.

```python
import jax
import jax.numpy as jnp
from jax import lax

D = 16384
FF = 26624
TOKENS = 64
N_COL = 8


def strengthened(result, rng, source, target, parts, factor):
    owner, partner = [(jnp.arange(result.shape[axis_at]) // (result.shape[axis_at] // parts)).reshape([-1 if axis == axis_at else 1 for axis in range(result.ndim)]) for axis_at in (source, target)]
    chosen = jax.random.permutation(rng, parts)[partner]
    strong = (owner == chosen) | (owner == (partner + parts // 2) % parts)
    return jnp.where(strong, factor * result, result)


def level_of(key, extent, shards, least, largest):
    gain, own = 1.0, jax.random.fold_in(key, 6)
    for dim, blocks in shards:
        heights = jnp.exp(jax.random.uniform(jax.random.fold_in(own, dim), (blocks,), jnp.float32, least / len(shards), largest / len(shards)))
        gain = gain * jnp.repeat(heights, extent[dim] // blocks).reshape([-1 if axis == dim else 1 for axis in range(len(extent))])
    return gain


def noise(key, shape, width, limit, pieces=(), held_as=jnp.bfloat16):
    loudness = level_of(key, shape, pieces, -0.22, 0.18) if pieces else 1.0
    drawn = jax.random.normal(key, shape, jnp.float32) * width * loudness
    return jnp.minimum(jnp.maximum(drawn, -limit), limit).astype(held_as)


def heavy_noise(key, extent, scale, reach, split, heavy, kind=jnp.bfloat16):
    entries = scale * jax.random.normal(key, extent, jnp.float32)
    if split:
        entries = entries * level_of(key, extent, split, -0.22, 0.18)
    return jnp.clip(strengthened(entries, jax.random.fold_in(key, 3), *heavy), -reach, reach).astype(kind)


def setup_inputs(seed: int = 0) -> dict:
    arg_keys = jax.random.split(jax.random.key(seed), 4)
    return {
        "tokens": heavy_noise(arg_keys[0], (TOKENS, D), 1.0, 6.0, ((0, 4), (1, 8)), (1, 0, 8, 2.0)),
        "gate_weight": noise(arg_keys[1], (D, FF), D ** -0.5, 0.046875, ((0, 8), (1, 4))),
        "up_weight": noise(arg_keys[2], (D, FF), D ** -0.5, 0.046875, ((0, 8), (1, 4))),
    }


def reference(tokens, gate_weight, up_weight):
    stride = D // N_COL

    def accumulate(totals, index):
        offset = (index * stride).astype(jnp.int32)
        feature_cols = lax.dynamic_slice_in_dim(tokens, offset, stride, 1)
        gate_block = lax.dynamic_slice_in_dim(gate_weight, offset, stride, 0)
        up_block = lax.dynamic_slice_in_dim(up_weight, offset, stride, 0)
        gate_part = jnp.dot(feature_cols, gate_block, preferred_element_type=jnp.float32)
        up_part = jnp.dot(feature_cols, up_block, preferred_element_type=jnp.float32)
        return (totals[0] + gate_part, totals[1] + up_part), None

    zeros = jnp.zeros((TOKENS, FF), jnp.float32)
    (gate, up), _ = lax.scan(accumulate, (zeros, zeros), jnp.arange(N_COL, dtype=jnp.int32))
    return (jax.nn.silu(gate) * up).astype(jnp.bfloat16)
```

```python
import functools

import jax
import jax.numpy as jnp
from jax import lax
from jax.experimental import pallas as pl
from jax.experimental.pallas import tpu as pltpu
from jax.sharding import PartitionSpec as P

MESH = pl.DeviceIdType.MESH

BUFFERS = 8
LAGS = (0, 4, 7, 10)
GATHER_LAG = 3
FAR = 4
SWAP_EVERY = 4
SWAP_AT = (1, 3)
WIDEST = 512


def digits_of(n):
    bits = n.bit_length() - 1
    return [(2**i, 2) for i in range(bits)]


LANES = 128
SPAN, FLOOR = 175.0, -87.0


def across(tile, width):
    return jnp.concatenate([tile] * (width // LANES), axis=1)


def encode(x, inverse):
    size = jnp.exp(jnp.abs(x) * across(inverse * SPAN, x.shape[1]) + FLOOR)
    return jnp.where(x < 0, -size, size).astype(jnp.bfloat16)


def decode(y, peak):
    y = y.astype(jnp.float32)
    size = (jnp.log(jnp.abs(y)) - FLOOR) * across(peak * (1.0 / SPAN), y.shape[1])
    return jnp.where(y < 0, -size, size)


def kernel(n_row, n_col, chunks, width, tok_hbm, gate_hbm, up_hbm, out, *scratch):
    stages = len(digits_of(n_col))
    direct = min(FAR, chunks)
    xg, wbuf, acc = scratch[0:3]
    held = scratch[3 : 2 + stages]
    scratch = scratch[2 + stages :]
    sends, recvs = scratch[:stages], scratch[stages : 2 * stages]
    tok_sem, tok_send, tok_recv, w_sem, far_send, far_recv = scratch[2 * stages : 2 * stages + 6]
    scratch = scratch[2 * stages + 6 :]
    rs_send, ag_send = scratch[:2]
    rs_recv, ag_recv = scratch[2 : 2 + stages], scratch[2 + stages :]

    row, col = lax.axis_index("row"), lax.axis_index("col")

    def weights(c, slot):
        cols = pl.ds(pl.multiple_of(c * width, width), width)
        return [
            pltpu.make_async_copy(hbm.at[:, cols], wbuf.at[slot, k], w_sem.at[slot, k])
            for k, hbm in enumerate((gate_hbm, up_hbm))
        ]

    own = pltpu.make_async_copy(tok_hbm, xg.at[row], tok_sem)
    own.start()

    barrier = pltpu.get_barrier_semaphore()
    greeted = 0
    for o in range(1, n_row):
        pl.semaphore_signal(barrier, inc=1, device_id=((row + o) % n_row, col), device_id_type=MESH)
        greeted += 1
    for o in range(1, n_col):
        pl.semaphore_signal(barrier, inc=1, device_id=(row, (col + o) % n_col), device_id_type=MESH)
        greeted += 1
    own.wait()
    for c in range(min(BUFFERS, chunks)):
        for copy in weights(c, c):
            copy.start()
    pl.semaphore_wait(barrier, greeted)

    def token_copy(o, place):
        return pltpu.make_async_remote_copy(
            src_ref=xg.at[place], dst_ref=xg.at[place], send_sem=tok_send.at[o - 1], recv_sem=tok_recv.at[o - 1],
            device_id=((row + o) % n_row, col), device_id_type=MESH)

    for o in range(1, n_row):
        token_copy(o, row).start()
    for o in range(1, n_row):
        token_copy(o, (row + n_row - o) % n_row).wait_recv()
    for o in range(1, n_row):
        token_copy(o, row).wait_send()

    low = lax.broadcasted_iota(jnp.int32, (xg.shape[0] * xg.shape[1] // n_col, LANES), 1) < LANES // 2

    places = [(col // weight) % 2 for weight, _ in digits_of(n_col)]
    weighed = [weight for weight, _ in digits_of(n_col)]

    def ordered(values, c):
        turn = c % SWAP_EVERY
        swapped = jnp.where(row % 2 == 0, turn == SWAP_AT[0], turn == SWAP_AT[1])
        first, second, *rest = values
        return [jnp.where(swapped, second, first), jnp.where(swapped, first, second), *rest]

    def peer(i, c):
        return (row, col + ((1 - 2 * ordered(places, c)[i]) * ordered(weighed, c)[i]))

    def rs_copy(i, c):
        return pltpu.make_async_remote_copy(
            src_ref=sends[i].at[c], dst_ref=recvs[i].at[c], send_sem=rs_send.at[i], recv_sem=rs_recv[i].at[c],
            device_id=peer(i, c), device_id_type=MESH)

    def coded(i, source, c):
        sub = source.shape[1] // 2
        to = 1 - ordered(places, c)[i]
        peaks = []
        for k in range(2):
            parts = [source[c, to * sub + g, k] for g in range(sub)]
            peak = functools.reduce(jnp.maximum, [
                jnp.abs(part[:, at : at + LANES]) for part in parts for at in range(0, width, LANES)])
            peak = jnp.maximum(peak, pltpu.roll(peak, LANES // 2, 1))
            peak = jnp.maximum(peak * 1.01, 1e-37).astype(jnp.bfloat16).astype(jnp.float32)
            peaks.append(peak)
            inverse = 1.0 / peak
            for g, part in enumerate(parts):
                at = (k * sub + g) * width
                sends[i][c, :, at : at + width] = encode(part, inverse)
        sends[i][c, :, 2 * sub * width :] = jnp.where(low, *peaks).astype(jnp.bfloat16)

    def summed(i, source, c, sink):
        sub = source.shape[1] // 2
        both = recvs[i][c, :, 2 * sub * width :].astype(jnp.float32)
        swapped = pltpu.roll(both, LANES // 2, 1)
        peaks = jnp.where(low, both, swapped), jnp.where(low, swapped, both)
        at_home = ordered(places, c)[i] * sub
        for k in range(2):
            for g in range(sub):
                at = (k * sub + g) * width
                total = source[c, at_home + g, k] + decode(recvs[i][c, :, at : at + width], peaks[k])
                sink(g, k, total)

    def cols(c):
        return pl.ds(pl.multiple_of(c * width, width), width)

    def block(values, c):
        index = 0
        for value in ordered(values, c):
            index = index * 2 + value
        return index

    def ag_copy(a, c, back):
        own = block(places, c) // 2**a
        start = (own + (1 - 2 * (own % 2)) if back else own) * 2**a
        ref = out.at[pl.ds(start, 2**a), :, cols(c)]
        return pltpu.make_async_remote_copy(
            src_ref=ref, dst_ref=ref, send_sem=ag_send.at[a], recv_sem=ag_recv[a].at[c],
            device_id=peer(stages - 1 - a, c), device_id_type=MESH)

    def far_copy(o, c):
        ref = out.at[block(places, c), :, cols(c)]
        return pltpu.make_async_remote_copy(
            src_ref=ref, dst_ref=ref, send_sem=far_send, recv_sem=far_recv,
            device_id=(row, (col + o) % n_col), device_id_type=MESH)

    def total_of(ref, sem):
        return pltpu.make_async_copy(ref, ref, sem)

    def arrived(s, c):
        if s == 0:
            for copy in weights(c, c % BUFFERS):
                copy.wait()
        else:
            rs_copy(s - 1, c).wait_recv()

    def worked(s, c):
        if s == 0:
            x = xg[...].reshape(-1, xg.shape[-1])
            for k in range(2):
                part = jnp.dot(x, wbuf[c % BUFFERS, k], preferred_element_type=jnp.float32)
                acc[c, :, k] = part.reshape(n_col, -1, width)
            coded(0, acc, c)
            return
        i = s - 1
        source = acc if i == 0 else held[i - 1]
        if i < stages - 1:
            def keep(g, k, total):
                held[i][c, g, k] = total

            summed(i, source, c, keep)
            coded(s, held[i], c)
        else:
            sums = []
            summed(i, source, c, lambda g, k, total: sums.append(total))
            gate, up = sums
            hidden = (gate / (1.0 + jnp.exp(-gate)) * up).astype(jnp.bfloat16)
            out[block(places, c), :, cols(c)] = hidden

    def sent(s, c):
        if s < stages:
            rs_copy(s, c).start()
        if s == 0:
            @pl.when(c + BUFFERS < chunks)
            def _():
                for copy in weights(c + BUFFERS, c % BUFFERS):
                    copy.start()
        if s == stages:
            @pl.when(c < chunks - direct)
            def _():
                ag_copy(0, c, False).start()

            @pl.when(c >= chunks - direct)
            def _():
                for o in range(1, n_col):
                    far_copy(o, c).start()

    def passed(a, c):
        @pl.when(jnp.logical_and(c >= 0, c < chunks - direct))
        def _():
            ag_copy(a, c, True).wait_recv()
            if a < stages - 1:
                ag_copy(a + 1, c, False).start()

    lags = (list(LAGS) + [LAGS[-1] + 3 * (i + 1) for i in range(stages)])[: 1 + stages]
    ag_lags = [lags[-1] + GATHER_LAG * (a + 1) for a in range(stages)]
    bounds = sorted({0, *lags, *[lag + chunks for lag in lags], chunks + ag_lags[-1]})
    for first, last in zip(bounds, bounds[1:]):
        active = [s for s, lag in enumerate(lags) if lag <= first < lag + chunks]

        def turn(t, carry, active=active):
            for act in (arrived, worked, sent):
                for s in active[::-1]:
                    act(s, t - lags[s])
            for a, lag in enumerate(ag_lags):
                passed(a, t - lag)
            return carry

        lax.fori_loop(first, last, turn, 0)

    for i in range(stages):
        total_of(sends[i], rs_send.at[i]).wait()
    near = (chunks - direct) * width
    if near:
        for a in range(stages):
            total_of(out.at[pl.ds(0, 2**a), :, pl.ds(0, near)], ag_send.at[a]).wait()
    if direct:
        far = out.at[pl.ds(0, n_col - 1), :, pl.ds(near, direct * width)]
        total_of(far, far_send).wait()
        total_of(far, far_recv).wait()


def solution(mesh):
    n_row, n_col = mesh.shape["row"], mesh.shape["col"]

    def local(tokens, gate_weight, up_weight):
        own_tokens, depth = tokens.shape
        columns = gate_weight.shape[1]
        each = own_tokens * n_row // n_col
        width = max(w for w in range(128, WIDEST + 1, 128) if columns % w == 0)
        chunks = columns // width
        digits = digits_of(n_col)
        radices = tuple(radix for _, radix in digits)
        subs, count = [], n_col
        for radix in radices:
            count //= radix
            subs.append(count)
        parts = [(chunks, each, 2 * sub * width + LANES) for sub in subs]
        scratch = [
            pltpu.VMEM((n_row, own_tokens, depth), jnp.bfloat16),
            pltpu.VMEM((BUFFERS, 2, depth, width), jnp.bfloat16),
            pltpu.VMEM((chunks, n_col, 2, each, width), jnp.float32),
        ]
        scratch += [pltpu.VMEM((chunks, sub, 2, each, width), jnp.float32) for sub in subs[:-1]]
        scratch += [pltpu.VMEM(shape, jnp.bfloat16) for shape in parts]
        scratch += [pltpu.VMEM(shape, jnp.bfloat16) for shape in parts]
        dma = pltpu.SemaphoreType.DMA
        scratch += [dma, dma((n_row - 1,)), dma((n_row - 1,)), dma((BUFFERS, 2))]
        scratch += [dma, dma, dma((len(digits),)), dma((len(digits),))]
        scratch += [dma((chunks,))] * len(digits) + [dma((max(chunks - FAR, 1),))] * len(digits)
        out = pl.pallas_call(
            functools.partial(kernel, n_row, n_col, chunks, width),
            out_shape=pltpu.VMEM((n_col, each, columns), jnp.bfloat16),
            in_specs=[pl.BlockSpec(memory_space=pl.ANY)] * 3,
            out_specs=pl.BlockSpec(memory_space=pltpu.VMEM),
            scratch_shapes=scratch,
            compiler_params=pltpu.CompilerParams(
                collective_id=0, has_side_effects=True, vmem_limit_bytes=56 * 2**20),
        )(tokens, gate_weight, up_weight)
        return out.reshape(n_col * each, columns)

    in_specs = (P("row", "col"), P("col", "row"), P("col", "row"))
    return jax.shard_map(local, mesh=mesh, in_specs=in_specs, out_specs=P(None, "row"), check_vma=False)
```

```python
import functools

import jax
import jax.numpy as jnp
from jax import lax
from jax.experimental import pallas as pl
from jax.experimental.pallas import tpu as pltpu
from jax.sharding import PartitionSpec as P

MESH = pl.DeviceIdType.MESH

BUFFERS = 8
LAGS = (0, 4, 8, 12)
GATHER_LAG = 3
FAR = (4, 2)
SWAP_EVERY = 4
SWAP_AT = (1, 3)
WIDEST = 512


def digits_of(n):
    bits = n.bit_length() - 1
    return [(2**i, 2) for i in range(bits)]


LANES = 128
SPAN, FLOOR = 175.0, -87.0


def across(tile, width):
    return jnp.concatenate([tile] * (width // LANES), axis=1)


def encode(x, inverse):
    size = jnp.exp(jnp.abs(x) * across(inverse * SPAN, x.shape[1]) + FLOOR)
    return jnp.where(x < 0, -size, size).astype(jnp.bfloat16)


def decode(y, peak):
    y = y.astype(jnp.float32)
    size = (jnp.log(jnp.abs(y)) - FLOOR) * across(peak * (1.0 / SPAN), y.shape[1])
    return jnp.where(y < 0, -size, size)


def kernel(n_row, n_col, chunks, width, tok_hbm, gate_hbm, up_hbm, out, *scratch):
    stages = len(digits_of(n_col))
    xg, wbuf, acc = scratch[0:3]
    held = scratch[3 : 2 + stages]
    scratch = scratch[2 + stages :]
    sends, recvs = scratch[:stages], scratch[stages : 2 * stages]
    tok_sem, tok_send, tok_recv, w_sem, far_send, far_recv = scratch[2 * stages : 2 * stages + 6]
    scratch = scratch[2 * stages + 6 :]
    rs_send, ag_send = scratch[:2]
    rs_recv, ag_recv = scratch[2 : 2 + stages], scratch[2 + stages :]

    row, col = lax.axis_index("row"), lax.axis_index("col")
    side = row % 2
    directs = [min(far, chunks) for far in FAR]
    direct = jnp.where(side == 0, *directs)

    def weights(c, slot):
        cols = pl.ds(pl.multiple_of(c * width, width), width)
        return [
            pltpu.make_async_copy(hbm.at[:, cols], wbuf.at[slot, k], w_sem.at[slot])
            for k, hbm in enumerate((gate_hbm, up_hbm))
        ]

    own = pltpu.make_async_copy(tok_hbm, xg.at[row], tok_sem)
    own.start()

    barrier = pltpu.get_barrier_semaphore()
    greeted = 0
    for o in range(1, n_row):
        pl.semaphore_signal(barrier, inc=1, device_id=((row + o) % n_row, col), device_id_type=MESH)
        greeted += 1
    for o in range(1, n_col):
        pl.semaphore_signal(barrier, inc=1, device_id=(row, (col + o) % n_col), device_id_type=MESH)
        greeted += 1
    own.wait()
    for c in range(min(BUFFERS, chunks)):
        for copy in weights(c, c):
            copy.start()
    pl.semaphore_wait(barrier, greeted)

    def total_of(ref, sem):
        return pltpu.make_async_copy(ref, ref, sem)

    for o in range(1, n_row):
        pltpu.make_async_remote_copy(
            src_ref=xg.at[row], dst_ref=xg.at[row], send_sem=tok_send, recv_sem=tok_recv,
            device_id=((row + o) % n_row, col), device_id_type=MESH).start()
    others = xg.at[pl.ds(0, n_row - 1)]
    total_of(others, tok_recv).wait()
    total_of(others, tok_send).wait()

    low = lax.broadcasted_iota(jnp.int32, (xg.shape[0] * xg.shape[1] // n_col, LANES), 1) < LANES // 2

    places = [(col // weight) % 2 for weight, _ in digits_of(n_col)]
    weighed = [weight for weight, _ in digits_of(n_col)]

    def ordered(values, c):
        turn = c % SWAP_EVERY
        swapped = jnp.where(row % 2 == 0, turn == SWAP_AT[0], turn == SWAP_AT[1])
        first, second, *rest = values
        return [jnp.where(swapped, second, first), jnp.where(swapped, first, second), *rest]

    def peer(i, c):
        return (row, col + ((1 - 2 * ordered(places, c)[i]) * ordered(weighed, c)[i]))

    def rs_copy(i, c):
        return pltpu.make_async_remote_copy(
            src_ref=sends[i].at[c], dst_ref=recvs[i].at[c], send_sem=rs_send.at[i], recv_sem=rs_recv[i].at[c],
            device_id=peer(i, c), device_id_type=MESH)

    def coded(i, source, c):
        sub = source.shape[1] // 2
        to = 1 - ordered(places, c)[i]
        peaks = []
        for k in range(2):
            parts = [source[c, to * sub + g, k] for g in range(sub)]
            peak = functools.reduce(jnp.maximum, [
                jnp.abs(part[:, at : at + LANES]) for part in parts for at in range(0, width, LANES)])
            peak = jnp.maximum(peak, pltpu.roll(peak, LANES // 2, 1))
            peak = jnp.maximum(peak * 1.01, 1e-37).astype(jnp.bfloat16).astype(jnp.float32)
            peaks.append(peak)
            inverse = 1.0 / peak
            for g, part in enumerate(parts):
                at = (k * sub + g) * width
                sends[i][c, :, at : at + width] = encode(part, inverse)
        sends[i][c, :, 2 * sub * width :] = jnp.where(low, *peaks).astype(jnp.bfloat16)

    def summed(i, source, c, sink):
        sub = source.shape[1] // 2
        both = recvs[i][c, :, 2 * sub * width :].astype(jnp.float32)
        swapped = pltpu.roll(both, LANES // 2, 1)
        peaks = jnp.where(low, both, swapped), jnp.where(low, swapped, both)
        at_home = ordered(places, c)[i] * sub
        for k in range(2):
            for g in range(sub):
                at = (k * sub + g) * width
                total = source[c, at_home + g, k] + decode(recvs[i][c, :, at : at + width], peaks[k])
                sink(g, k, total)

    def cols(c):
        return pl.ds(pl.multiple_of(c * width, width), width)

    def block(values, c):
        index = 0
        for value in ordered(values, c):
            index = index * 2 + value
        return index

    def ag_copy(a, c, back):
        own = block(places, c) // 2**a
        start = (own + (1 - 2 * (own % 2)) if back else own) * 2**a
        ref = out.at[pl.ds(start, 2**a), :, cols(c)]
        return pltpu.make_async_remote_copy(
            src_ref=ref, dst_ref=ref, send_sem=ag_send.at[a], recv_sem=ag_recv[a].at[c if a < stages - 1 else 0],
            device_id=peer(stages - 1 - a, c), device_id_type=MESH)

    def far_copy(o, c):
        ref = out.at[block(places, c), :, cols(c)]
        return pltpu.make_async_remote_copy(
            src_ref=ref, dst_ref=ref, send_sem=far_send, recv_sem=far_recv,
            device_id=(row, (col + o) % n_col), device_id_type=MESH)

    def arrived(s, c):
        if s == 0:
            total_of(wbuf.at[c % BUFFERS], w_sem.at[c % BUFFERS]).wait()
        else:
            rs_copy(s - 1, c).wait_recv()

    def worked(s, c):
        if s == 0:
            x = xg[...].reshape(-1, xg.shape[-1])
            for k in range(2):
                part = jnp.dot(x, wbuf[c % BUFFERS, k], preferred_element_type=jnp.float32)
                acc[c, :, k] = part.reshape(n_col, -1, width)
            coded(0, acc, c)
            return
        i = s - 1
        source = acc if i == 0 else held[i - 1]
        if i < stages - 1:
            def keep(g, k, total):
                held[i][c, g, k] = total

            summed(i, source, c, keep)
            coded(s, held[i], c)
        else:
            sums = []
            summed(i, source, c, lambda g, k, total: sums.append(total))
            gate, up = sums
            hidden = (gate / (1.0 + jnp.exp(-gate)) * up).astype(jnp.bfloat16)
            out[block(places, c), :, cols(c)] = hidden

    def sent(s, c):
        if s < stages:
            rs_copy(s, c).start()
        if s == 0:
            @pl.when(c + BUFFERS < chunks)
            def _():
                for copy in weights(c + BUFFERS, c % BUFFERS):
                    copy.start()
        if s == stages:
            @pl.when(c < chunks - direct)
            def _():
                ag_copy(0, c, False).start()

            @pl.when(c >= chunks - direct)
            def _():
                for o in range(1, n_col):
                    far_copy(o, c).start()

    def passed(a, c):
        @pl.when(jnp.logical_and(c >= 0, c < chunks - direct))
        def _():
            ag_copy(a, c, True).wait_recv()
            ag_copy(a + 1, c, False).start()

    lags = (list(LAGS) + [LAGS[-1] + 3 * (i + 1) for i in range(stages)])[: 1 + stages]
    ag_lags = [lags[-1] + GATHER_LAG * (a + 1) for a in range(stages - 1)]
    bounds = sorted({0, *lags, *[lag + chunks for lag in lags], chunks + ag_lags[-1]})
    for first, last in zip(bounds, bounds[1:]):
        active = [s for s, lag in enumerate(lags) if lag <= first < lag + chunks]

        def turn(t, carry, active=active):
            for act in (arrived, worked, sent):
                for s in active[::-1]:
                    act(s, t - lags[s])
            for a, lag in enumerate(ag_lags):
                passed(a, t - lag)
            return carry

        lax.fori_loop(first, last, turn, 0)

    for i in range(stages):
        total_of(sends[i], rs_send.at[i]).wait()
    for which, far in enumerate(directs):
        @pl.when(side == which)
        def _(far=far):
            near = (chunks - far) * width
            if near:
                for a in range(stages):
                    total_of(out.at[pl.ds(0, 2**a), :, pl.ds(0, near)], ag_send.at[a]).wait()
                total_of(out.at[pl.ds(0, n_col // 2), :, pl.ds(0, near)], ag_recv[-1].at[0]).wait()
            if far:
                ref = out.at[pl.ds(0, n_col - 1), :, pl.ds(near, far * width)]
                total_of(ref, far_send).wait()
                total_of(ref, far_recv).wait()


def solution(mesh):
    n_row, n_col = mesh.shape["row"], mesh.shape["col"]

    def local(tokens, gate_weight, up_weight):
        own_tokens, depth = tokens.shape
        columns = gate_weight.shape[1]
        each = own_tokens * n_row // n_col
        width = max(w for w in range(128, WIDEST + 1, 128) if columns % w == 0)
        chunks = columns // width
        digits = digits_of(n_col)
        radices = tuple(radix for _, radix in digits)
        subs, count = [], n_col
        for radix in radices:
            count //= radix
            subs.append(count)
        parts = [(chunks, each, 2 * sub * width + LANES) for sub in subs]
        scratch = [
            pltpu.VMEM((n_row, own_tokens, depth), jnp.bfloat16),
            pltpu.VMEM((BUFFERS, 2, depth, width), jnp.bfloat16),
            pltpu.VMEM((chunks, n_col, 2, each, width), jnp.float32),
        ]
        scratch += [pltpu.VMEM((chunks, sub, 2, each, width), jnp.float32) for sub in subs[:-1]]
        scratch += [pltpu.VMEM(shape, jnp.bfloat16) for shape in parts]
        scratch += [pltpu.VMEM(shape, jnp.bfloat16) for shape in parts]
        dma = pltpu.SemaphoreType.DMA
        scratch += [dma, dma, dma, dma((BUFFERS,))]
        scratch += [dma, dma, dma((len(digits),)), dma((len(digits),))]
        scratch += [dma((chunks,))] * len(digits) + [dma((max(chunks - min(FAR), 1),))] * (len(digits) - 1) + [dma((1,))]
        out = pl.pallas_call(
            functools.partial(kernel, n_row, n_col, chunks, width),
            out_shape=pltpu.VMEM((n_col, each, columns), jnp.bfloat16),
            in_specs=[pl.BlockSpec(memory_space=pl.ANY)] * 3,
            out_specs=pl.BlockSpec(memory_space=pltpu.VMEM),
            scratch_shapes=scratch,
            compiler_params=pltpu.CompilerParams(
                collective_id=0, has_side_effects=True, vmem_limit_bytes=56 * 2**20),
        )(tokens, gate_weight, up_weight)
        return out.reshape(n_col * each, columns)

    in_specs = (P("row", "col"), P("col", "row"), P("col", "row"))
    return jax.shard_map(local, mesh=mesh, in_specs=in_specs, out_specs=P(None, "row"), check_vma=False)
```

```python
import functools

import jax
import jax.numpy as jnp
from jax import lax
from jax.experimental import pallas as pl
from jax.experimental.pallas import tpu as pltpu
from jax.sharding import PartitionSpec as P

MESH = pl.DeviceIdType.MESH

BUFFERS = 8
LAGS = (0, 4, 8, 12)
GATHER_LAG = 3
FAR = (4, 2)
SWAP_EVERY = 4
SWAP_AT = (1, 3)
WIDEST = 512


def digits_of(n):
    bits = n.bit_length() - 1
    return [(2**i, 2) for i in range(bits)]


LANES = 128
SPAN, FLOOR = 175.0, -87.0


def across(tile, width):
    return jnp.concatenate([tile] * (width // LANES), axis=1)


def encode(x, inverse):
    size = jnp.exp(jnp.abs(x) * across(inverse * SPAN, x.shape[1]) + FLOOR)
    return jnp.where(x < 0, -size, size).astype(jnp.bfloat16)


def decode(y, peak):
    y = y.astype(jnp.float32)
    size = (jnp.log(jnp.abs(y)) - FLOOR) * across(peak * (1.0 / SPAN), y.shape[1])
    return jnp.where(y < 0, -size, size)


def kernel(n_row, n_col, chunks, width, tok_hbm, gate_hbm, up_hbm, out, *scratch):
    stages = len(digits_of(n_col))
    xg, wbuf, acc = scratch[0:3]
    held = scratch[3 : 2 + stages]
    scratch = scratch[2 + stages :]
    sends, recvs = scratch[:stages], scratch[stages : 2 * stages]
    tok_sem, tok_send, tok_recv, w_sem, far_send, far_recv = scratch[2 * stages : 2 * stages + 6]
    scratch = scratch[2 * stages + 6 :]
    rs_send, ag_send = scratch[:2]
    rs_recv, ag_recv = scratch[2 : 2 + stages], scratch[2 + stages :]

    row, col = lax.axis_index("row"), lax.axis_index("col")
    side = row % 2
    directs = [min(far, chunks) for far in FAR]
    direct = jnp.where(side == 0, *directs)

    def weights(c, slot):
        cols = pl.ds(pl.multiple_of(c * width, width), width)
        return [
            pltpu.make_async_copy(hbm.at[:, cols], wbuf.at[slot, k], w_sem.at[slot])
            for k, hbm in enumerate((gate_hbm, up_hbm))
        ]

    own = pltpu.make_async_copy(tok_hbm, xg.at[row], tok_sem)
    own.start()

    barrier = pltpu.get_barrier_semaphore()
    greeted = 0
    for o in range(1, n_row):
        pl.semaphore_signal(barrier, inc=1, device_id=((row + o) % n_row, col), device_id_type=MESH)
        greeted += 1
    for o in range(1, n_col):
        pl.semaphore_signal(barrier, inc=1, device_id=(row, (col + o) % n_col), device_id_type=MESH)
        greeted += 1
    own.wait()
    for c in range(min(BUFFERS, chunks)):
        for copy in weights(c, c):
            copy.start()
    pl.semaphore_wait(barrier, greeted)

    def total_of(ref, sem):
        return pltpu.make_async_copy(ref, ref, sem)

    for o in range(1, n_row):
        pltpu.make_async_remote_copy(
            src_ref=xg.at[row], dst_ref=xg.at[row], send_sem=tok_send, recv_sem=tok_recv,
            device_id=((row + o) % n_row, col), device_id_type=MESH).start()
    others = xg.at[pl.ds(0, n_row - 1)]
    total_of(others, tok_recv).wait()
    total_of(others, tok_send).wait()

    low = lax.broadcasted_iota(jnp.int32, (xg.shape[0] * xg.shape[1] // n_col, LANES), 1) < LANES // 2

    places = [(col // weight) % 2 for weight, _ in digits_of(n_col)]
    weighed = [weight for weight, _ in digits_of(n_col)]

    def ordered(values, c):
        turn = c % SWAP_EVERY
        swapped = jnp.where(row % 2 == 0, turn == SWAP_AT[0], turn == SWAP_AT[1])
        first, second, *rest = values
        return [jnp.where(swapped, second, first), jnp.where(swapped, first, second), *rest]

    def peer(i, c):
        return (row, col + ((1 - 2 * ordered(places, c)[i]) * ordered(weighed, c)[i]))

    def rs_copy(i, c):
        return pltpu.make_async_remote_copy(
            src_ref=sends[i].at[c], dst_ref=recvs[i].at[c], send_sem=rs_send.at[i], recv_sem=rs_recv[i].at[c],
            device_id=peer(i, c), device_id_type=MESH)

    def coded(i, source, c):
        sub = source.shape[1] // 2
        to = 1 - ordered(places, c)[i]
        peaks = []
        for k in range(2):
            parts = [source[c, to * sub + g, k] for g in range(sub)]
            peak = functools.reduce(jnp.maximum, [
                jnp.abs(part[:, at : at + LANES]) for part in parts for at in range(0, width, LANES)])
            peak = jnp.maximum(peak, pltpu.roll(peak, LANES // 2, 1))
            peak = jnp.maximum(peak * 1.01, 1e-37).astype(jnp.bfloat16).astype(jnp.float32)
            peaks.append(peak)
            inverse = 1.0 / peak
            for g, part in enumerate(parts):
                at = (k * sub + g) * width
                sends[i][c, :, at : at + width] = encode(part, inverse)
        sends[i][c, :, 2 * sub * width :] = jnp.where(low, *peaks).astype(jnp.bfloat16)

    def summed(i, source, c, sink):
        sub = source.shape[1] // 2
        both = recvs[i][c, :, 2 * sub * width :].astype(jnp.float32)
        swapped = pltpu.roll(both, LANES // 2, 1)
        peaks = jnp.where(low, both, swapped), jnp.where(low, swapped, both)
        at_home = ordered(places, c)[i] * sub
        for k in range(2):
            for g in range(sub):
                at = (k * sub + g) * width
                total = source[c, at_home + g, k] + decode(recvs[i][c, :, at : at + width], peaks[k])
                sink(g, k, total)

    def cols(c):
        return pl.ds(pl.multiple_of(c * width, width), width)

    def block(values, c):
        index = 0
        for value in ordered(values, c):
            index = index * 2 + value
        return index

    def ag_copy(a, c, back):
        own = block(places, c) // 2**a
        start = (own + (1 - 2 * (own % 2)) if back else own) * 2**a
        ref = out.at[pl.ds(start, 2**a), :, cols(c)]
        return pltpu.make_async_remote_copy(
            src_ref=ref, dst_ref=ref, send_sem=ag_send.at[a], recv_sem=ag_recv[a].at[c if a < stages - 1 else 0],
            device_id=peer(stages - 1 - a, c), device_id_type=MESH)

    def far_copy(o, c):
        ref = out.at[block(places, c), :, cols(c)]
        return pltpu.make_async_remote_copy(
            src_ref=ref, dst_ref=ref, send_sem=far_send, recv_sem=far_recv,
            device_id=(row, (col + o) % n_col), device_id_type=MESH)

    def arrived(s, c):
        if s == 0:
            total_of(wbuf.at[c % BUFFERS], w_sem.at[c % BUFFERS]).wait()
        else:
            rs_copy(s - 1, c).wait_recv()

    def worked(s, c):
        if s == 0:
            x = xg[...].reshape(-1, xg.shape[-1])
            for k in range(2):
                part = jnp.dot(x, wbuf[c % BUFFERS, k], preferred_element_type=jnp.float32)
                acc[c, :, k] = part.reshape(n_col, -1, width)
            coded(0, acc, c)
            return
        i = s - 1
        source = acc if i == 0 else held[i - 1]
        if i < stages - 1:
            def keep(g, k, total):
                held[i][c, g, k] = total

            summed(i, source, c, keep)
            coded(s, held[i], c)
        else:
            sums = []
            summed(i, source, c, lambda g, k, total: sums.append(total))
            gate, up = sums
            hidden = (gate / (1.0 + jnp.exp(-gate)) * up).astype(jnp.bfloat16)
            out[block(places, c), :, cols(c)] = hidden

    def sent(s, c):
        if s < stages:
            rs_copy(s, c).start()
        if s == 0:
            @pl.when(c + BUFFERS < chunks)
            def _():
                for copy in weights(c + BUFFERS, c % BUFFERS):
                    copy.start()
        if s == stages:
            @pl.when(c < chunks - direct)
            def _():
                ag_copy(0, c, False).start()

            @pl.when(c >= chunks - direct)
            def _():
                for o in range(1, n_col)[::-1]:
                    far_copy(o, c).start()

    def passed(a, c):
        @pl.when(jnp.logical_and(c >= 0, c < chunks - direct))
        def _():
            ag_copy(a, c, True).wait_recv()
            ag_copy(a + 1, c, False).start()

    lags = (list(LAGS) + [LAGS[-1] + 3 * (i + 1) for i in range(stages)])[: 1 + stages]
    ag_lags = [lags[-1] + GATHER_LAG * (a + 1) for a in range(stages - 1)]
    bounds = sorted({0, *lags, *[lag + chunks for lag in lags], chunks + ag_lags[-1]})
    for first, last in zip(bounds, bounds[1:]):
        active = [s for s, lag in enumerate(lags) if lag <= first < lag + chunks]

        def turn(t, carry, active=active):
            for act in (arrived, worked, sent):
                for s in active[::-1]:
                    act(s, t - lags[s])
            for a, lag in enumerate(ag_lags):
                passed(a, t - lag)
            return carry

        lax.fori_loop(first, last, turn, 0)

    for i in range(stages):
        total_of(sends[i], rs_send.at[i]).wait()
    for which, far in enumerate(directs):
        @pl.when(side == which)
        def _(far=far):
            near = (chunks - far) * width
            if near:
                for a in range(stages):
                    total_of(out.at[pl.ds(0, 2**a), :, pl.ds(0, near)], ag_send.at[a]).wait()
                total_of(out.at[pl.ds(0, n_col // 2), :, pl.ds(0, near)], ag_recv[-1].at[0]).wait()
            if far:
                ref = out.at[pl.ds(0, n_col - 1), :, pl.ds(near, far * width)]
                total_of(ref, far_send).wait()
                total_of(ref, far_recv).wait()


def solution(mesh):
    n_row, n_col = mesh.shape["row"], mesh.shape["col"]

    def local(tokens, gate_weight, up_weight):
        own_tokens, depth = tokens.shape
        columns = gate_weight.shape[1]
        each = own_tokens * n_row // n_col
        width = max(w for w in range(128, WIDEST + 1, 128) if columns % w == 0)
        chunks = columns // width
        digits = digits_of(n_col)
        radices = tuple(radix for _, radix in digits)
        subs, count = [], n_col
        for radix in radices:
            count //= radix
            subs.append(count)
        parts = [(chunks, each, 2 * sub * width + LANES) for sub in subs]
        scratch = [
            pltpu.VMEM((n_row, own_tokens, depth), jnp.bfloat16),
            pltpu.VMEM((BUFFERS, 2, depth, width), jnp.bfloat16),
            pltpu.VMEM((chunks, n_col, 2, each, width), jnp.float32),
        ]
        scratch += [pltpu.VMEM((chunks, sub, 2, each, width), jnp.float32) for sub in subs[:-1]]
        scratch += [pltpu.VMEM(shape, jnp.bfloat16) for shape in parts]
        scratch += [pltpu.VMEM(shape, jnp.bfloat16) for shape in parts]
        dma = pltpu.SemaphoreType.DMA
        scratch += [dma, dma, dma, dma((BUFFERS,))]
        scratch += [dma, dma, dma((len(digits),)), dma((len(digits),))]
        scratch += [dma((chunks,))] * len(digits) + [dma((max(chunks - min(FAR), 1),))] * (len(digits) - 1) + [dma((1,))]
        out = pl.pallas_call(
            functools.partial(kernel, n_row, n_col, chunks, width),
            out_shape=pltpu.VMEM((n_col, each, columns), jnp.bfloat16),
            in_specs=[pl.BlockSpec(memory_space=pl.ANY)] * 3,
            out_specs=pl.BlockSpec(memory_space=pltpu.VMEM),
            scratch_shapes=scratch,
            compiler_params=pltpu.CompilerParams(
                collective_id=0, has_side_effects=True, vmem_limit_bytes=56 * 2**20),
        )(tokens, gate_weight, up_weight)
        return out.reshape(n_col * each, columns)

    in_specs = (P("row", "col"), P("col", "row"), P("col", "row"))
    return jax.shard_map(local, mesh=mesh, in_specs=in_specs, out_specs=P(None, "row"), check_vma=False)
```
